32 devices in a mesh: batch: 1 (over z), py: 4 (over y), px: 8 (over x, core).
Axes of the slice: x: 4, y: 4, z: 1, core: 2. Of those that a mesh axis runs over, the one named last changes fastest.
The devices are a block of a 4x4x8 slice.
Arguments:
- pair_rep: bfloat16 [1024, 1024, 64], P(('batch', 'px'), 'py')
- pair_mask: int32 [1024, 1024], P(('batch', 'px'), 'py')
- ln_in: bfloat16 [2, 2, 64], replicated
- w_in: bfloat16 [2, 64, 320], replicated
- b_in: bfloat16 [2, 320], replicated
- ln_out: bfloat16 [2, 2, 64], replicated
- w_out: bfloat16 [2, 64, 64], replicated
- b_out: bfloat16 [2, 64], replicated
Outputs:
- output: bfloat16 [1024, 1024, 64], P(('batch', 'px'), 'py')
All inputs are finite; a program needn't handle non-finite values.
Results may differ from the reference program's by a relative error of at most 0.00639573.
Values are sent between devices in bfloat16 or wider.
A program may use at most 768 MiB of HBM per device.

```python
import jax
import jax.numpy as jnp
from jax import lax

RESIDUES = 1024
PAIR_DIM = 64
HIDDEN_DIM = 64
ROW_BLOCK = min(RESIDUES, 64)
NUM_BLOCKS = RESIDUES // ROW_BLOCK
CHAN_GROUP = min(HIDDEN_DIM, 16)
NUM_GROUPS = HIDDEN_DIM // CHAN_GROUP
LN_EPS = 1e-5


def setup_inputs(seed: int = 0, part: int = 0) -> dict:
    base_key = jax.random.key(seed)
    part_key = jax.random.fold_in(base_key, part)
    key_pair, key_len = jax.random.split(part_key, 2)
    weight_keys = jax.random.split(jax.random.key(seed + 1), 6)
    in_width = 4 * HIDDEN_DIM + PAIR_DIM
    pair_rep = jax.random.normal(key_pair, (RESIDUES, RESIDUES, PAIR_DIM), jnp.float32).astype(jnp.bfloat16)
    length = RESIDUES - jax.random.randint(key_len, (), 0, RESIDUES // 4 + 1)
    valid = (jnp.arange(RESIDUES) < length).astype(jnp.int32)
    pair_mask = valid[:, None] * valid[None, :]
    ln_base = jnp.array([1.0, 0.0], jnp.float32)[None, :, None]
    ln_in = (ln_base + 0.3 * jax.random.normal(weight_keys[0], (2, 2, PAIR_DIM), jnp.float32)).astype(jnp.bfloat16)
    w_in = (jax.random.normal(weight_keys[1], (2, PAIR_DIM, in_width), jnp.float32) * PAIR_DIM ** -0.5).astype(jnp.bfloat16)
    b_in = (0.5 * jax.random.normal(weight_keys[2], (2, in_width), jnp.float32)).astype(jnp.bfloat16)
    ln_out = (ln_base + 0.3 * jax.random.normal(weight_keys[3], (2, 2, HIDDEN_DIM), jnp.float32)).astype(jnp.bfloat16)
    w_out = (jax.random.normal(weight_keys[4], (2, HIDDEN_DIM, PAIR_DIM), jnp.float32) * HIDDEN_DIM ** -0.5).astype(jnp.bfloat16)
    b_out = (0.5 * jax.random.normal(weight_keys[5], (2, PAIR_DIM), jnp.float32)).astype(jnp.bfloat16)
    return {'pair_rep': pair_rep, 'pair_mask': pair_mask, 'ln_in': ln_in, 'w_in': w_in, 'b_in': b_in, 'ln_out': ln_out, 'w_out': w_out, 'b_out': b_out}


def layer_norm(values, ln_gain, ln_shift, norm_axis):
    average = jnp.mean(values, axis=norm_axis, keepdims=True)
    centered = values - average
    variance = jnp.mean(centered * centered, axis=norm_axis, keepdims=True)
    return centered * lax.rsqrt(variance + LN_EPS) * ln_gain + ln_shift


def norm_pairs(pair_rows, ln_in):
    normed = layer_norm(pair_rows.astype(jnp.float32), ln_in[0].astype(jnp.float32), ln_in[1].astype(jnp.float32), -1)
    return normed.astype(jnp.bfloat16)


def gated_operands(pair_rows, mask_rows, ln_in, w_in, b_in):
    proj_width = 4 * HIDDEN_DIM
    normed = norm_pairs(pair_rows, ln_in)
    projected = jnp.einsum('ijd,de->eij', normed.astype(jnp.float32), w_in[:, :proj_width].astype(jnp.float32))
    projected = projected + b_in[:proj_width].astype(jnp.float32)[:, None, None]
    projected = projected.reshape(4, HIDDEN_DIM, ROW_BLOCK, RESIDUES)
    mask_f32 = mask_rows.astype(jnp.float32)[None]
    left_op = mask_f32 * jax.nn.sigmoid(projected[0]) * projected[1]
    right_op = mask_f32 * jax.nn.sigmoid(projected[2]) * projected[3]
    return left_op.astype(jnp.bfloat16), right_op.astype(jnp.bfloat16)


def tri_update(pair_rep, pair_mask, ln_in, w_in, b_in, ln_out, w_out, b_out, outgoing):
    proj_width = 4 * HIDDEN_DIM
    pair_blocks = pair_rep.reshape(NUM_BLOCKS, ROW_BLOCK, RESIDUES, PAIR_DIM)
    mask_blocks = pair_mask.reshape(NUM_BLOCKS, ROW_BLOCK, RESIDUES)
    left_blocks, right_blocks = lax.map(lambda block_in: gated_operands(block_in[0], block_in[1], ln_in, w_in, b_in), (pair_blocks, mask_blocks))
    left_full = left_blocks.transpose(1, 0, 2, 3).reshape(HIDDEN_DIM, RESIDUES, RESIDUES)
    right_full = right_blocks.transpose(1, 0, 2, 3).reshape(HIDDEN_DIM, RESIDUES, RESIDUES)
    right_groups = right_full.reshape(NUM_GROUPS, CHAN_GROUP, RESIDUES, RESIDUES)
    if outgoing:
        left_sel = left_full.reshape(HIDDEN_DIM, NUM_BLOCKS, ROW_BLOCK, RESIDUES).transpose(1, 0, 2, 3)
        left_sel = left_sel.reshape(NUM_BLOCKS, NUM_GROUPS, CHAN_GROUP, ROW_BLOCK, RESIDUES)
        sum_form = 'cik,cjk->cij'
    else:
        left_sel = left_full.reshape(HIDDEN_DIM, RESIDUES, NUM_BLOCKS, ROW_BLOCK).transpose(2, 0, 1, 3)
        left_sel = left_sel.reshape(NUM_BLOCKS, NUM_GROUPS, CHAN_GROUP, RESIDUES, ROW_BLOCK)
        sum_form = 'cki,ckj->cij'
    gain_out = ln_out[0].astype(jnp.float32)[:, None, None]
    shift_out = ln_out[1].astype(jnp.float32)[:, None, None]

    def group_product(group_pair):
        return jnp.einsum(sum_form, group_pair[0].astype(jnp.float32), group_pair[1].astype(jnp.float32))

    def block_update(block_in):
        pair_rows, left_groups = block_in
        tri_sum = lax.map(group_product, (left_groups, right_groups)).reshape(HIDDEN_DIM, ROW_BLOCK, RESIDUES)
        normed_sum = layer_norm(tri_sum, gain_out, shift_out, 0).astype(jnp.bfloat16)
        update = jnp.einsum('cij,cd->ijd', normed_sum.astype(jnp.float32), w_out.astype(jnp.float32))
        update = update + b_out.astype(jnp.float32)
        normed = norm_pairs(pair_rows, ln_in)
        gate_val = jax.nn.sigmoid(jnp.einsum('ijd,de->ije', normed.astype(jnp.float32), w_in[:, proj_width:].astype(jnp.float32)) + b_in[proj_width:].astype(jnp.float32))
        return (pair_rows.astype(jnp.float32) + gate_val * update).astype(jnp.bfloat16)

    new_blocks = lax.map(block_update, (pair_blocks, left_sel))
    return new_blocks.reshape(RESIDUES, RESIDUES, PAIR_DIM)


def reference(pair_rep, pair_mask, ln_in, w_in, b_in, ln_out, w_out, b_out):
    after_out = tri_update(pair_rep, pair_mask, ln_in[0], w_in[0], b_in[0], ln_out[0], w_out[0], b_out[0], True)
    return tri_update(after_out, pair_mask, ln_in[1], w_in[1], b_in[1], ln_out[1], w_out[1], b_out[1], False)
```

```python
import functools

import jax
import jax.numpy as jnp
from jax import lax
from jax.experimental import pallas as pl
from jax.experimental.pallas import tpu as pltpu
from jax.sharding import PartitionSpec as P

LN_EPS = 1e-5
SUB = 8
GATE_ROWS = 4
MESH = pl.DeviceIdType.MESH
BF16 = jnp.bfloat16
F32 = jnp.float32


def dot(lhs, rhs, dims=((1,), (0,))):
    return lax.dot_general(lhs, rhs, (dims, ((), ())), preferred_element_type=F32)


def tree_sum(parts):
    while len(parts) > 1:
        parts = [parts[k] + parts[k + 1] if k + 1 < len(parts) else parts[k] for k in range(0, len(parts), 2)]
    return parts[0]


def kernel(npy, npx, z_ref, mask_ref, wab_ref, bab_ref, ln_in_ref, wg_ref, bg_ref, ln_out_ref, wo_ref, bo_ref,
           out_ref, zn, proj, xn, ab_out, ab_in, a_t, x_out, x_in,
           ab_ss, ab_rs, x_ss, x_rs, free_sem):
    rows, dim, cols = z_ref.shape
    hidden = x_in.shape[0]
    n = npy * npx
    slots = hidden // n
    full = npx * rows
    tile = 2 * rows
    my_py, my_px = lax.axis_index('py'), lax.axis_index('px')
    my_x, my_core = my_px // 2, lax.rem(my_px, 2)
    nx = npx // 2

    def peer(off):
        f, t, e = off
        dpy = lax.rem(my_py + f, npy)
        dpx = 2 * lax.rem(my_x + t, nx) + lax.rem(my_core + e, 2)
        return dpy, dpx

    def lin(dev):
        return dev[0] * npx + dev[1]

    def dev_id(dev):
        return {'py': dev[0], 'px': dev[1]}

    me = (my_py, my_px)
    here = lin(me)
    offsets = [((s + s // nx) % npy, s % nx, e) for s in range(npy * nx) for e in range(2)]
    others = [o for o in offsets if o != (0, 0, 0)]

    def at_rows(dev):
        return pl.ds(pl.multiple_of(dev[1] * rows, rows), rows)

    def at_cols(dev):
        return pl.ds(pl.multiple_of(dev[0] * cols, cols), cols)

    def ab_copy(s, src, dst):
        return pltpu.make_async_remote_copy(
            src_ref=ab_out.at[s, lin(dst)], dst_ref=ab_in.at[s, :, at_rows(src), at_cols(src)],
            send_sem=ab_ss.at[s, lin(dst)], recv_sem=ab_rs.at[s, lin(src)],
            device_id=dev_id(dst), device_id_type=MESH)

    def x_copy(s, src, dst):
        return pltpu.make_async_remote_copy(
            src_ref=x_out.at[s, at_rows(dst), at_cols(dst)], dst_ref=x_in.at[s * n + lin(src)],
            send_sem=x_ss.at[s, lin(dst)], recv_sem=x_rs.at[s, lin(src)],
            device_id=dev_id(dst), device_id_type=MESH)

    def normalize(src_ref, u):
        gain, shift = ln_in_ref[u, 0], ln_in_ref[u, 1]

        @pl.loop(0, rows)
        def _(i):
            for h in range(cols // 128):
                lanes = pl.ds(h * 128, 128)
                val = src_ref[i, :, lanes].astype(F32)
                cen = val - jnp.mean(val, axis=0, keepdims=True)
                var = jnp.mean(cen * cen, axis=0, keepdims=True)
                zn[i, :, lanes] = (cen * lax.rsqrt(var + LN_EPS) * gain + shift).astype(BF16)

    def project(u, s):
        @pl.loop(0, rows // (2 * SUB))
        def _(g):
            for h in range(2):
                rhs = zn[pl.ds(g * 2 * SUB + h * SUB, SUB)].reshape(SUB * dim, cols)
                proj[h, pl.ds(0, 4 * n * SUB), :] = dot(wab_ref[u, s], rhs)
            at = pl.ds(pl.multiple_of(g * 2 * SUB, 2 * SUB), 2 * SUB)
            mask = mask_ref[at, :].astype(F32)

            @pl.loop(0, n, unroll=2)
            def _(d):
                for op in range(2):
                    bias_g, bias_p = bab_ref[u, s, 2 * op, d], bab_ref[u, s, 2 * op + 1, d]
                    g_at = pl.ds(pl.multiple_of((2 * op * n + d) * SUB, SUB), SUB)
                    p_at = pl.ds(pl.multiple_of(((2 * op + 1) * n + d) * SUB, SUB), SUB)
                    gate = jnp.concatenate([proj[0, g_at, :], proj[1, g_at, :]], axis=0) + bias_g
                    lin_p = jnp.concatenate([proj[0, p_at, :], proj[1, p_at, :]], axis=0) + bias_p
                    ab_out[s, d, op, at, :] = (mask * jax.nn.sigmoid(gate) * lin_p).astype(BF16)

    def send_ab(s):
        for off in others:
            ab_copy(s, me, peer(off)).start()
        ab_in[s, :, at_rows(me), at_cols(me)] = ab_out[s, here]

    def products(u, s):
        for t in range(nx):
            m = lax.rem(my_x + t, nx)
            m_at = pl.ds(pl.multiple_of(m * tile, tile), tile)
            if u == 0:
                lhs_ref = ab_in.at[s, 0, m_at, :]
            else:
                a_t[...] = ab_in[s, 0, :, m_at].T
                lhs_ref = a_t

            @pl.loop(0, full // cols)
            def _(q):
                q_at = pl.ds(pl.multiple_of(q * cols, cols), cols)
                if u == 0:
                    x_out[s, m_at, q_at] = dot(lhs_ref[...], ab_in[s, 1, q_at, :], ((1,), (1,)))
                else:
                    x_out[s, m_at, q_at] = dot(lhs_ref[...], ab_in[s, 1, :, q_at])

            for off in offsets:
                if off[1] == t:
                    if off == (0, 0, 0):
                        x_in[s * n + here] = x_out[s, at_rows(me), at_cols(me)]
                    else:
                        x_copy(s, me, peer(off)).start()

    def finish(src_ref, u):
        @pl.loop(0, rows // SUB)
        def _(g):
            at = pl.ds(pl.multiple_of(g * SUB, SUB), SUB)
            for h in range(cols // 128):
                lanes = pl.ds(h * 128, 128)
                avg = tree_sum([x_in[c, at, lanes] for c in range(hidden)]) * (1.0 / hidden)
                var = tree_sum([jnp.square(x_in[c, at, lanes] - avg) for c in range(hidden)]) * (1.0 / hidden)
                inv = lax.rsqrt(var + LN_EPS)
                for c in range(0, hidden, 2):
                    pair = [(x_in[k, at, lanes] - avg) * inv * ln_out_ref[u, 0, k] + ln_out_ref[u, 1, k] for k in (c, c + 1)]
                    xn[pl.ds(c * SUB, 2 * SUB), lanes] = jnp.concatenate(pair, axis=0).astype(BF16)
            proj[0, pl.ds(0, SUB * dim), :] = dot(wo_ref[u], xn[...])
            for k in range(SUB // GATE_ROWS):
                rhs = zn[pl.ds(g * SUB + k * GATE_ROWS, GATE_ROWS)].reshape(GATE_ROWS * dim, cols)
                proj[1, pl.ds(k * GATE_ROWS * dim, GATE_ROWS * dim), :] = dot(wg_ref[u], rhs)

            @pl.loop(0, SUB)
            def _(r):
                r_at = pl.ds(pl.multiple_of(r * dim, dim), dim)
                for h in range(cols // 128):
                    lanes = pl.ds(h * 128, 128)
                    gate = jax.nn.sigmoid(proj[1, r_at, lanes] + bg_ref[u])
                    upd = proj[0, r_at, lanes] + bo_ref[u]
                    out_ref[g * SUB + r, :, lanes] = (src_ref[g * SUB + r, :, lanes].astype(F32) + gate * upd).astype(BF16)

    barrier = pltpu.get_barrier_semaphore()
    for off in others:
        pl.semaphore_signal(barrier, inc=1, device_id=dev_id(peer(off)), device_id_type=MESH)
    normalize(z_ref, 0)
    pl.semaphore_wait(barrier, n - 1)

    for u in range(2):
        src_ref = z_ref if u == 0 else out_ref
        if u == 1:
            normalize(src_ref, u)
            for s in range(slots):
                for off in others:
                    ab_copy(s, me, peer(off)).wait_send()
            pl.semaphore_wait(free_sem, n - 1)
        for s in range(slots):
            project(u, s)
            send_ab(s)
        for s in range(slots):
            for off in others:
                ab_copy(s, peer(off), me).wait_recv()
            if u == 1:
                for off in others:
                    x_copy(s, me, peer(off)).wait_send()
            products(u, s)
        if u == 0:
            for off in others:
                pl.semaphore_signal(free_sem, inc=1, device_id=dev_id(peer(off)), device_id_type=MESH)
        for s in range(slots):
            for off in others:
                x_copy(s, peer(off), me).wait_recv()
        finish(src_ref, u)
    for s in range(slots):
        for off in others:
            ab_copy(s, me, peer(off)).wait_send()
            x_copy(s, me, peer(off)).wait_send()


def solution(mesh):
    pair_spec = P(('batch', 'px'), 'py', None)
    mask_spec = P(('batch', 'px'), 'py')
    whole = P()
    npy, npx = mesh.shape['py'], mesh.shape['px']
    n = npy * npx

    def device_body(pair_blk, mask_blk, ln_in, w_in, b_in, ln_out, w_out, b_out):
        rows, cols, dim = pair_blk.shape
        hidden = w_out.shape[1]
        slots = hidden // n
        full = npx * rows
        updates = w_in.shape[0]
        zero = jnp.zeros((), BF16)
        eye8 = jnp.eye(SUB, dtype=jnp.bool_)
        eye4 = jnp.eye(GATE_ROWS, dtype=jnp.bool_)

        w_t = jnp.swapaxes(w_in, 1, 2)
        wab = w_t[:, :4 * hidden].reshape(updates, 4, slots, n, dim).transpose(0, 2, 1, 3, 4)
        wab = wab.reshape(updates, slots, 4 * n, 1, 1, dim)
        wab = jnp.where(eye8[:, :, None], wab, zero).reshape(updates, slots, 4 * n * SUB, SUB * dim)
        bab = b_in[:, :4 * hidden].astype(F32).reshape(updates, 4, slots, n).transpose(0, 2, 1, 3)
        wg = w_t[:, 4 * hidden:].reshape(updates, 1, dim, 1, dim)
        wg = jnp.where(eye4[:, None, :, None], wg, zero).reshape(updates, GATE_ROWS * dim, GATE_ROWS * dim)
        wo = jnp.swapaxes(w_out, 1, 2).reshape(updates, 1, dim, hidden, 1)
        wo = jnp.where(eye8[:, None, None, :], wo, zero).reshape(updates, SUB * dim, SUB * hidden)
        bg = jnp.broadcast_to(b_in[:, 4 * hidden:, None].astype(F32), (updates, dim, 128))
        bo = jnp.broadcast_to(b_out[:, :, None].astype(F32), (updates, dim, 128))
        ln_i = jnp.broadcast_to(ln_in[:, :, :, None].astype(F32), (updates, 2, dim, 128))
        ln_o = jnp.broadcast_to(ln_out[:, :, :, None, None].astype(F32), (updates, 2, hidden, SUB, 128))

        vmem = pl.BlockSpec(memory_space=pltpu.VMEM)
        smem = pl.BlockSpec(memory_space=pltpu.SMEM)
        out = pl.pallas_call(
            functools.partial(kernel, npy, npx),
            out_shape=jax.ShapeDtypeStruct((rows, dim, cols), BF16),
            in_specs=[vmem, vmem, vmem, smem] + [vmem] * 6,
            out_specs=vmem,
            scratch_shapes=[
                pltpu.VMEM((rows, dim, cols), BF16),
                pltpu.VMEM((2, SUB * max(4 * n, dim), cols), F32),
                pltpu.VMEM((SUB * hidden, cols), BF16),
                pltpu.VMEM((slots, n, 2, rows, cols), BF16),
                pltpu.VMEM((slots, 2, full, full), BF16),
                pltpu.VMEM((2 * rows, full), BF16),
                pltpu.VMEM((slots, full, full), F32),
                pltpu.VMEM((hidden, rows, cols), F32),
                pltpu.SemaphoreType.DMA((slots, n)),
                pltpu.SemaphoreType.DMA((slots, n)),
                pltpu.SemaphoreType.DMA((slots, n)),
                pltpu.SemaphoreType.DMA((slots, n)),
                pltpu.SemaphoreType.REGULAR,
            ],
            compiler_params=pltpu.CompilerParams(collective_id=0, has_side_effects=True, vmem_limit_bytes=67043328),
            name='triangle',
        )(jnp.swapaxes(pair_blk, 1, 2), mask_blk, wab, bab, ln_i, wg, bg, ln_o, wo, bo)
        return jnp.swapaxes(out, 1, 2)

    return jax.shard_map(device_body, mesh=mesh, in_specs=(pair_spec, mask_spec, whole, whole, whole, whole, whole, whole), out_specs=pair_spec, check_vma=False)
```

```python
import functools

import jax
import jax.numpy as jnp
from jax import lax
from jax.experimental import pallas as pl
from jax.experimental.pallas import tpu as pltpu
from jax.sharding import PartitionSpec as P

LN_EPS = 1e-5
SUB = 8
GATE_ROWS = 4
MESH = pl.DeviceIdType.MESH
BF16 = jnp.bfloat16
F32 = jnp.float32


def dot(lhs, rhs, dims=((1,), (0,))):
    return lax.dot_general(lhs, rhs, (dims, ((), ())), preferred_element_type=F32)


def tree_sum(parts):
    while len(parts) > 1:
        parts = [parts[k] + parts[k + 1] if k + 1 < len(parts) else parts[k] for k in range(0, len(parts), 2)]
    return parts[0]


def kernel(npy, npx, z_ref, mask_ref, w_in_ref, w_out_ref, bias_ref, vec_ref,
           out_ref, w_t, wab, wg, wo, zn, proj, xn, ab_out, ab_in, a_t, x_out, x_in,
           ab_ss, ab_rs, x_ss, x_rs, free_sem):
    rows, dim, cols = z_ref.shape
    hidden = x_in.shape[0]
    width = w_in_ref.shape[2]
    n = npy * npx
    slots = hidden // n
    full = npx * rows
    tile = 2 * rows
    my_py, my_px = lax.axis_index('py'), lax.axis_index('px')
    my_x, my_core = my_px // 2, lax.rem(my_px, 2)
    nx = npx // 2

    def peer(off):
        f, t, e = off
        dpy = lax.rem(my_py + f, npy)
        dpx = 2 * lax.rem(my_x + t, nx) + lax.rem(my_core + e, 2)
        return dpy, dpx

    def lin(dev):
        return dev[0] * npx + dev[1]

    def dev_id(dev):
        return {'py': dev[0], 'px': dev[1]}

    me = (my_py, my_px)
    here = lin(me)
    def reach(off):
        hops = [min(off[0], npy - off[0]), min(off[1], nx - off[1])]
        halfway = 2 * off[0] == npy or 2 * off[1] == nx
        return halfway, sum(hops)

    diagonal = [((k + k // nx) % npy, k % nx, e) for k in range(npy * nx) for e in range(2)]
    others = sorted([off for off in diagonal if off != (0, 0, 0)], key=reach)

    def at_rows(dev):
        return pl.ds(pl.multiple_of(dev[1] * rows, rows), rows)

    def at_cols(dev):
        return pl.ds(pl.multiple_of(dev[0] * cols, cols), cols)

    def ab_copy(s, src, dst):
        return pltpu.make_async_remote_copy(
            src_ref=ab_out.at[s, lin(dst)], dst_ref=ab_in.at[s, :, at_rows(src), at_cols(src)],
            send_sem=ab_ss.at[s, lin(dst)], recv_sem=ab_rs.at[s, lin(src)],
            device_id=dev_id(dst), device_id_type=MESH)

    def x_copy(s, src, dst):
        return pltpu.make_async_remote_copy(
            src_ref=x_out.at[s, at_rows(dst), at_cols(dst)], dst_ref=x_in.at[s * n + lin(src)],
            send_sem=x_ss.at[s, lin(dst)], recv_sem=x_rs.at[s, lin(src)],
            device_id=dev_id(dst), device_id_type=MESH)

    def iota(shape, axis):
        return lax.broadcasted_iota(jnp.int32, shape, axis)

    def spread_weights(u):
        wide = (dim, SUB * dim)
        pick = (lax.rem(iota(wide, 1), dim) == iota(wide, 0)).astype(F32).astype(BF16)
        w_t[...] = dot(w_in_ref[u], pick, ((0,), (0,))).astype(BF16)
        big = (n * SUB, SUB * dim)
        keep = lax.rem(iota(big, 0), SUB) == iota(big, 1) // dim
        sel = (n * SUB, width)
        for s in range(slots):
            for k in range(4):
                first = k * hidden + s * n
                rep = (iota(sel, 0) // SUB + first == iota(sel, 1)).astype(F32).astype(BF16)
                wab[s, pl.ds(k * n * SUB, n * SUB), :] = jnp.where(keep, dot(rep, w_t[...]), 0.0).astype(BF16)
        gate_w = w_t[pl.ds(4 * hidden, dim), pl.ds(0, GATE_ROWS * dim)].astype(F32)
        lane = iota(gate_w.shape, 1)
        for r in range(GATE_ROWS):
            wg[pl.ds(r * dim, dim), :] = jnp.where(lane // dim == r, gate_w, 0.0).astype(BF16)
        wide = (hidden, SUB * hidden)
        pick = (iota(wide, 1) // SUB == iota(wide, 0)).astype(F32).astype(BF16)
        out_w = dot(w_out_ref[u], pick, ((0,), (0,)))
        lane = iota(out_w.shape, 1)
        for r in range(SUB):
            wo[pl.ds(r * dim, dim), :] = jnp.where(lax.rem(lane, SUB) == r, out_w, 0.0).astype(BF16)

    def normalize(src_ref, u):
        gain, shift = vec_ref[u, 0], vec_ref[u, 1]

        @pl.loop(0, rows)
        def _(i):
            for h in range(cols // 128):
                lanes = pl.ds(h * 128, 128)
                val = src_ref[i, :, lanes].astype(F32)
                cen = val - jnp.mean(val, axis=0, keepdims=True)
                var = jnp.mean(cen * cen, axis=0, keepdims=True)
                zn[i, :, lanes] = (cen * lax.rsqrt(var + LN_EPS) * gain + shift).astype(BF16)

    def project(u, s):
        @pl.loop(0, rows // (2 * SUB))
        def _(g):
            for h in range(2):
                rhs = zn[pl.ds(g * 2 * SUB + h * SUB, SUB)].reshape(SUB * dim, cols)
                proj[h, pl.ds(0, 4 * n * SUB), :] = dot(wab[s], rhs)
            at = pl.ds(pl.multiple_of(g * 2 * SUB, 2 * SUB), 2 * SUB)
            mask = mask_ref[at, :].astype(F32)

            @pl.loop(0, n, unroll=2)
            def _(d):
                for op in range(2):
                    bias_g, bias_p = bias_ref[u, 2 * op * hidden + s * n + d], bias_ref[u, (2 * op + 1) * hidden + s * n + d]
                    g_at = pl.ds(pl.multiple_of((2 * op * n + d) * SUB, SUB), SUB)
                    p_at = pl.ds(pl.multiple_of(((2 * op + 1) * n + d) * SUB, SUB), SUB)
                    gate = jnp.concatenate([proj[0, g_at, :], proj[1, g_at, :]], axis=0) + bias_g
                    lin_p = jnp.concatenate([proj[0, p_at, :], proj[1, p_at, :]], axis=0) + bias_p
                    ab_out[s, d, op, at, :] = (mask * jax.nn.sigmoid(gate) * lin_p).astype(BF16)

    def send_ab(s):
        for off in others:
            ab_copy(s, me, peer(off)).start()
        ab_in[s, :, at_rows(me), at_cols(me)] = ab_out[s, here]

    def products(u, s):
        for t in range(nx):
            m = lax.rem(my_x + t, nx)
            m_at = pl.ds(pl.multiple_of(m * tile, tile), tile)
            if u == 0:
                lhs_ref = ab_in.at[s, 0, m_at, :]
            else:
                a_t[...] = ab_in[s, 0, :, m_at].T
                lhs_ref = a_t

            @pl.loop(0, full // cols)
            def _(q):
                q_at = pl.ds(pl.multiple_of(q * cols, cols), cols)
                if u == 0:
                    x_out[s, m_at, q_at] = dot(lhs_ref[...], ab_in[s, 1, q_at, :], ((1,), (1,)))
                else:
                    x_out[s, m_at, q_at] = dot(lhs_ref[...], ab_in[s, 1, :, q_at])

        for off in others:
            x_copy(s, me, peer(off)).start()
        x_in[s * n + here] = x_out[s, at_rows(me), at_cols(me)]

    def finish(src_ref, u):
        @pl.loop(0, rows // SUB)
        def _(g):
            at = pl.ds(pl.multiple_of(g * SUB, SUB), SUB)
            for h in range(cols // 128):
                lanes = pl.ds(h * 128, 128)
                avg = tree_sum([x_in[c, at, lanes] for c in range(hidden)]) * (1.0 / hidden)
                var = tree_sum([jnp.square(x_in[c, at, lanes] - avg) for c in range(hidden)]) * (1.0 / hidden)
                inv = lax.rsqrt(var + LN_EPS)
                for c in range(0, hidden, 2):
                    pair = [(x_in[k, at, lanes] - avg) * inv * vec_ref[u, 4, pl.ds(k, 1), :] + vec_ref[u, 5, pl.ds(k, 1), :] for k in (c, c + 1)]
                    xn[pl.ds(c * SUB, 2 * SUB), lanes] = jnp.concatenate(pair, axis=0).astype(BF16)
            proj[0, pl.ds(0, SUB * dim), :] = dot(wo[...], xn[...])
            for k in range(SUB // GATE_ROWS):
                rhs = zn[pl.ds(g * SUB + k * GATE_ROWS, GATE_ROWS)].reshape(GATE_ROWS * dim, cols)
                proj[1, pl.ds(k * GATE_ROWS * dim, GATE_ROWS * dim), :] = dot(wg[...], rhs)

            @pl.loop(0, SUB)
            def _(r):
                r_at = pl.ds(pl.multiple_of(r * dim, dim), dim)
                for h in range(cols // 128):
                    lanes = pl.ds(h * 128, 128)
                    gate = jax.nn.sigmoid(proj[1, r_at, lanes] + vec_ref[u, 2])
                    upd = proj[0, r_at, lanes] + vec_ref[u, 3]
                    out_ref[g * SUB + r, :, lanes] = (src_ref[g * SUB + r, :, lanes].astype(F32) + gate * upd).astype(BF16)

    barrier = pltpu.get_barrier_semaphore()
    for off in others:
        pl.semaphore_signal(barrier, inc=1, device_id=dev_id(peer(off)), device_id_type=MESH)
    spread_weights(0)
    normalize(z_ref, 0)
    pl.semaphore_wait(barrier, n - 1)

    for u in range(2):
        src_ref = z_ref if u == 0 else out_ref
        if u == 1:
            spread_weights(u)
            normalize(src_ref, u)
            for s in range(slots):
                for off in others:
                    ab_copy(s, me, peer(off)).wait_send()
            pl.semaphore_wait(free_sem, n - 1)
        for s in range(slots):
            project(u, s)
            send_ab(s)
        for s in range(slots):
            for off in others:
                ab_copy(s, peer(off), me).wait_recv()
            if u == 1:
                for off in others:
                    x_copy(s, me, peer(off)).wait_send()
            products(u, s)
        if u == 0:
            for off in others:
                pl.semaphore_signal(free_sem, inc=1, device_id=dev_id(peer(off)), device_id_type=MESH)
        for s in range(slots):
            for off in others:
                x_copy(s, peer(off), me).wait_recv()
        finish(src_ref, u)
    for s in range(slots):
        for off in others:
            ab_copy(s, me, peer(off)).wait_send()
            x_copy(s, me, peer(off)).wait_send()


def solution(mesh):
    pair_spec = P(('batch', 'px'), 'py', None)
    mask_spec = P(('batch', 'px'), 'py')
    whole = P()
    npy, npx = mesh.shape['py'], mesh.shape['px']
    n = npy * npx

    def device_body(pair_blk, mask_blk, ln_in, w_in, b_in, ln_out, w_out, b_out):
        rows, cols, dim = pair_blk.shape
        hidden = w_out.shape[1]
        slots = hidden // n
        full = npx * rows
        width = w_in.shape[2]
        gate_at = 4 * hidden
        vec = jnp.concatenate([ln_in, b_in[:, None, gate_at:], b_out[:, None], ln_out], axis=1)
        vec = jnp.broadcast_to(vec.astype(F32)[..., None], (*vec.shape, 128))
        bias = b_in.astype(F32)

        vmem = pl.BlockSpec(memory_space=pltpu.VMEM)
        smem = pl.BlockSpec(memory_space=pltpu.SMEM)
        out = pl.pallas_call(
            functools.partial(kernel, npy, npx),
            out_shape=jax.ShapeDtypeStruct((rows, dim, cols), BF16),
            in_specs=[vmem, vmem, vmem, vmem, smem, vmem],
            out_specs=vmem,
            scratch_shapes=[
                pltpu.VMEM((width, SUB * dim), BF16),
                pltpu.VMEM((slots, 4 * n * SUB, SUB * dim), BF16),
                pltpu.VMEM((GATE_ROWS * dim, GATE_ROWS * dim), BF16),
                pltpu.VMEM((SUB * dim, SUB * hidden), BF16),
                pltpu.VMEM((rows, dim, cols), BF16),
                pltpu.VMEM((2, SUB * max(4 * n, dim), cols), F32),
                pltpu.VMEM((SUB * hidden, cols), BF16),
                pltpu.VMEM((slots, n, 2, rows, cols), BF16),
                pltpu.VMEM((slots, 2, full, full), BF16),
                pltpu.VMEM((2 * rows, full), BF16),
                pltpu.VMEM((slots, full, full), F32),
                pltpu.VMEM((hidden, rows, cols), F32),
                pltpu.SemaphoreType.DMA((slots, n)),
                pltpu.SemaphoreType.DMA((slots, n)),
                pltpu.SemaphoreType.DMA((slots, n)),
                pltpu.SemaphoreType.DMA((slots, n)),
                pltpu.SemaphoreType.REGULAR,
            ],
            compiler_params=pltpu.CompilerParams(collective_id=0, has_side_effects=True, vmem_limit_bytes=67043328),
            name='triangle',
        )(jnp.swapaxes(pair_blk, 1, 2), mask_blk, w_in, w_out, bias, vec)
        return jnp.swapaxes(out, 1, 2)

    return jax.shard_map(device_body, mesh=mesh, in_specs=(pair_spec, mask_spec, whole, whole, whole, whole, whole, whole), out_specs=pair_spec, check_vma=False)
```

```python
import functools

import jax
import jax.numpy as jnp
from jax import lax
from jax.experimental import pallas as pl
from jax.experimental.pallas import tpu as pltpu
from jax.sharding import PartitionSpec as P

LN_EPS = 1e-5
SUB = 8
GATE_ROWS = 4
MESH = pl.DeviceIdType.MESH
BF16 = jnp.bfloat16
F32 = jnp.float32


def dot(lhs, rhs, dims=((1,), (0,))):
    return lax.dot_general(lhs, rhs, (dims, ((), ())), preferred_element_type=F32)


def tree_sum(parts):
    while len(parts) > 1:
        parts = [parts[k] + parts[k + 1] if k + 1 < len(parts) else parts[k] for k in range(0, len(parts), 2)]
    return parts[0]


def kernel(npy, npx, z_ref, mask_ref, w_in_ref, w_out_ref, bias_ref, vec_ref,
           out_ref, w_t, wab, wg, wo, zn, proj, xn, ab_out, ab_in, a_t, x_out, x_in,
           ab_hop, x_hop, ab_ss, ab_rs, x_ss, x_rs, ab_hr, ab_fs, x_hr, x_fs, free_sem):
    rows, dim, cols = z_ref.shape
    hidden = x_in.shape[0]
    width = w_in_ref.shape[2]
    n = npy * npx
    slots = hidden // n
    full = npx * rows
    tile = 2 * rows
    my_py, my_px = lax.axis_index('py'), lax.axis_index('px')
    my_x, my_core = my_px // 2, lax.rem(my_px, 2)
    nx = npx // 2

    def peer(off):
        f, t, e = off
        dpy = lax.rem(my_py + f, npy)
        dpx = 2 * lax.rem(my_x + t, nx) + lax.rem(my_core + e, 2)
        return dpy, dpx

    def lin(dev):
        return dev[0] * npx + dev[1]

    def dev_id(dev):
        return {'py': dev[0], 'px': dev[1]}

    me = (my_py, my_px)
    here = lin(me)
    def halfway(off):
        return (npy > 2 and 2 * off[0] == npy) or (nx > 2 and 2 * off[1] == nx)

    diagonal = [((k + k // nx) % npy, k % nx, e) for k in range(npy * nx) for e in range(2)]
    others = [off for off in diagonal if off != (0, 0, 0)]
    near = [off for off in others if not halfway(off)]
    far = [off for off in others if halfway(off)]

    def legs(s, off):
        f, t, e = off
        turn = 1 if (s + e) % 2 == 0 else -1
        f1 = turn % npy if npy > 2 and 2 * f == npy else f
        t1 = turn % nx if nx > 2 and 2 * t == nx else t
        return (f1, t1, e), ((f - f1) % npy, (t - t1) % nx, 0)

    def each_other(body):
        @pl.loop(1, n)
        def _(k):
            dev = lax.rem(here + k, n)
            body((dev // npx, lax.rem(dev, npx)))

    def signal_all(sem):
        each_other(lambda dev: pl.semaphore_signal(sem, inc=1, device_id=dev_id(dev), device_id_type=MESH))

    def back(off):
        return (-off[0]) % npy, (-off[1]) % nx, off[2]

    def at_rows(dev):
        return pl.ds(pl.multiple_of(dev[1] * rows, rows), rows)

    def at_cols(dev):
        return pl.ds(pl.multiple_of(dev[0] * cols, cols), cols)

    def ab_copy(s, src, dst):
        return pltpu.make_async_remote_copy(
            src_ref=ab_out.at[s, lin(dst)], dst_ref=ab_in.at[s, :, at_rows(src), at_cols(src)],
            send_sem=ab_ss.at[s, lin(dst)], recv_sem=ab_rs.at[s, lin(src)],
            device_id=dev_id(dst), device_id_type=MESH)

    def x_copy(s, src, dst):
        return pltpu.make_async_remote_copy(
            src_ref=x_out.at[s, at_rows(dst), at_cols(dst)], dst_ref=x_in.at[s * n + lin(src)],
            send_sem=x_ss.at[s, lin(dst)], recv_sem=x_rs.at[s, lin(src)],
            device_id=dev_id(dst), device_id_type=MESH)

    def remote(src, dst, send_sem, recv_sem, dev):
        return pltpu.make_async_remote_copy(src_ref=src, dst_ref=dst, send_sem=send_sem, recv_sem=recv_sem,
                                            device_id=dev_id(dev), device_id_type=MESH)

    def ab_first(s, k):
        return remote(ab_out.at[s, lin(peer(far[k]))], ab_hop.at[s, k], ab_ss.at[s, lin(peer(far[k]))], ab_hr.at[s, k],
                      peer(legs(s, far[k])[0]))

    def ab_second(s, k):
        first, second = legs(s, far[k])
        src = peer(back(first))
        return remote(ab_hop.at[s, k], ab_in.at[s, :, at_rows(src), at_cols(src)], ab_fs.at[s, k], ab_rs.at[s, lin(src)], peer(second))

    def x_first(s, k):
        dst = peer(far[k])
        return remote(x_out.at[s, at_rows(dst), at_cols(dst)], x_hop.at[s, k], x_ss.at[s, lin(dst)], x_hr.at[s, k],
                      peer(legs(s, far[k])[0]))

    def x_second(s, k):
        first, second = legs(s, far[k])
        src = peer(back(first))
        return remote(x_hop.at[s, k], x_in.at[s * n + lin(src)], x_fs.at[s, k], x_rs.at[s, lin(src)], peer(second))

    def ab_left(s, k):
        return remote(ab_hop.at[s, k], ab_in.at[s, :, at_rows(me), at_cols(me)], ab_fs.at[s, k], ab_rs.at[s, here], me)

    def x_left(s, k):
        return remote(x_hop.at[s, k], x_in.at[s * n + here], x_fs.at[s, k], x_rs.at[s, here], me)

    def pass_on(first, second, s):
        for k in range(len(far)):
            first(s, k).wait_recv()
            second(s, k).start()

    def iota(shape, axis):
        return lax.broadcasted_iota(jnp.int32, shape, axis)

    def spread_weights(u):
        wide = (dim, SUB * dim)
        pick = (lax.rem(iota(wide, 1), dim) == iota(wide, 0)).astype(F32).astype(BF16)
        w_t[...] = dot(w_in_ref[u], pick, ((0,), (0,))).astype(BF16)
        big = (n * SUB, SUB * dim)
        keep = lax.rem(iota(big, 0), SUB) == iota(big, 1) // dim
        sel = (n * SUB, width)
        for s in range(slots):
            for k in range(4):
                first = k * hidden + s * n
                rep = (iota(sel, 0) // SUB + first == iota(sel, 1)).astype(F32).astype(BF16)
                wab[s, pl.ds(k * n * SUB, n * SUB), :] = jnp.where(keep, dot(rep, w_t[...]), 0.0).astype(BF16)
        gate_w = w_t[pl.ds(4 * hidden, dim), pl.ds(0, GATE_ROWS * dim)].astype(F32)
        lane = iota(gate_w.shape, 1)
        for r in range(GATE_ROWS):
            wg[pl.ds(r * dim, dim), :] = jnp.where(lane // dim == r, gate_w, 0.0).astype(BF16)
        wide = (hidden, SUB * hidden)
        pick = (iota(wide, 1) // SUB == iota(wide, 0)).astype(F32).astype(BF16)
        out_w = dot(w_out_ref[u], pick, ((0,), (0,)))
        lane = iota(out_w.shape, 1)
        for r in range(SUB):
            wo[pl.ds(r * dim, dim), :] = jnp.where(lax.rem(lane, SUB) == r, out_w, 0.0).astype(BF16)

    def normalize(src_ref, u):
        gain, shift = vec_ref[u, 0], vec_ref[u, 1]

        @pl.loop(0, rows)
        def _(i):
            for h in range(cols // 128):
                lanes = pl.ds(h * 128, 128)
                val = src_ref[i, :, lanes].astype(F32)
                cen = val - jnp.mean(val, axis=0, keepdims=True)
                var = jnp.mean(cen * cen, axis=0, keepdims=True)
                zn[i, :, lanes] = (cen * lax.rsqrt(var + LN_EPS) * gain + shift).astype(BF16)

    def project(u, s):
        @pl.loop(0, rows // (2 * SUB))
        def _(g):
            for h in range(2):
                rhs = zn[pl.ds(g * 2 * SUB + h * SUB, SUB)].reshape(SUB * dim, cols)
                proj[h, pl.ds(0, 4 * n * SUB), :] = dot(wab[s], rhs)
            at = pl.ds(pl.multiple_of(g * 2 * SUB, 2 * SUB), 2 * SUB)
            mask = mask_ref[at, :].astype(F32)

            @pl.loop(0, n, unroll=2)
            def _(d):
                for op in range(2):
                    bias_g, bias_p = bias_ref[u, 2 * op * hidden + s * n + d], bias_ref[u, (2 * op + 1) * hidden + s * n + d]
                    g_at = pl.ds(pl.multiple_of((2 * op * n + d) * SUB, SUB), SUB)
                    p_at = pl.ds(pl.multiple_of(((2 * op + 1) * n + d) * SUB, SUB), SUB)
                    gate = jnp.concatenate([proj[0, g_at, :], proj[1, g_at, :]], axis=0) + bias_g
                    lin_p = jnp.concatenate([proj[0, p_at, :], proj[1, p_at, :]], axis=0) + bias_p
                    ab_out[s, d, op, at, :] = (mask * jax.nn.sigmoid(gate) * lin_p).astype(BF16)

    def send_ab(s):
        for k in range(len(far)):
            ab_first(s, k).start()
        for off in near:
            ab_copy(s, me, peer(off)).start()
        ab_in[s, :, at_rows(me), at_cols(me)] = ab_out[s, here]

    def products(u, s):
        for t in range(nx):
            m = lax.rem(my_x + t, nx)
            m_at = pl.ds(pl.multiple_of(m * tile, tile), tile)
            if u == 0:
                lhs_ref = ab_in.at[s, 0, m_at, :]
            else:
                a_t[...] = ab_in[s, 0, :, m_at].T
                lhs_ref = a_t

            @pl.loop(0, full // cols)
            def _(q):
                q_at = pl.ds(pl.multiple_of(q * cols, cols), cols)
                if u == 0:
                    x_out[s, m_at, q_at] = dot(lhs_ref[...], ab_in[s, 1, q_at, :], ((1,), (1,)))
                else:
                    x_out[s, m_at, q_at] = dot(lhs_ref[...], ab_in[s, 1, :, q_at])

        for k in range(len(far)):
            x_first(s, k).start()
        for off in near:
            x_copy(s, me, peer(off)).start()
        x_in[s * n + here] = x_out[s, at_rows(me), at_cols(me)]

    def finish(src_ref, u):
        @pl.loop(0, rows // SUB)
        def _(g):
            at = pl.ds(pl.multiple_of(g * SUB, SUB), SUB)
            for h in range(cols // 128):
                lanes = pl.ds(h * 128, 128)
                avg = tree_sum([x_in[c, at, lanes] for c in range(hidden)]) * (1.0 / hidden)
                var = tree_sum([jnp.square(x_in[c, at, lanes] - avg) for c in range(hidden)]) * (1.0 / hidden)
                inv = lax.rsqrt(var + LN_EPS)
                for c in range(0, hidden, 2):
                    pair = [(x_in[k, at, lanes] - avg) * inv * vec_ref[u, 4, pl.ds(k, 1), :] + vec_ref[u, 5, pl.ds(k, 1), :] for k in (c, c + 1)]
                    xn[pl.ds(c * SUB, 2 * SUB), lanes] = jnp.concatenate(pair, axis=0).astype(BF16)
            proj[0, pl.ds(0, SUB * dim), :] = dot(wo[...], xn[...])
            for k in range(SUB // GATE_ROWS):
                rhs = zn[pl.ds(g * SUB + k * GATE_ROWS, GATE_ROWS)].reshape(GATE_ROWS * dim, cols)
                proj[1, pl.ds(k * GATE_ROWS * dim, GATE_ROWS * dim), :] = dot(wg[...], rhs)

            @pl.loop(0, SUB)
            def _(r):
                r_at = pl.ds(pl.multiple_of(r * dim, dim), dim)
                for h in range(cols // 128):
                    lanes = pl.ds(h * 128, 128)
                    gate = jax.nn.sigmoid(proj[1, r_at, lanes] + vec_ref[u, 2])
                    upd = proj[0, r_at, lanes] + vec_ref[u, 3]
                    out_ref[g * SUB + r, :, lanes] = (src_ref[g * SUB + r, :, lanes].astype(F32) + gate * upd).astype(BF16)

    barrier = pltpu.get_barrier_semaphore()
    signal_all(barrier)
    spread_weights(0)
    normalize(z_ref, 0)
    pl.semaphore_wait(barrier, n - 1)

    def wait_forwards(second):
        for s in range(slots):
            @pl.loop(0, len(far))
            def _(k):
                second(s, k).wait_send()

    for u in range(2):
        src_ref = z_ref if u == 0 else out_ref
        if u == 1:
            spread_weights(u)
            normalize(src_ref, u)
            for s in range(slots):
                each_other(lambda dev: ab_copy(s, me, dev).wait_send())
            wait_forwards(x_left)
            pl.semaphore_wait(free_sem, n - 1)
        for s in range(slots):
            project(u, s)
            send_ab(s)
        for s in range(slots):
            pass_on(ab_first, ab_second, s)
            each_other(lambda dev: ab_copy(s, dev, me).wait_recv())
            if u == 1:
                each_other(lambda dev: x_copy(s, me, dev).wait_send())
            products(u, s)
        wait_forwards(ab_left)
        if u == 0:
            signal_all(free_sem)
        for s in range(slots):
            pass_on(x_first, x_second, s)
        for s in range(slots):
            each_other(lambda dev: x_copy(s, dev, me).wait_recv())
        finish(src_ref, u)
    for s in range(slots):
        each_other(lambda dev: ab_copy(s, me, dev).wait_send())
        each_other(lambda dev: x_copy(s, me, dev).wait_send())
    wait_forwards(x_left)


def solution(mesh):
    pair_spec = P(('batch', 'px'), 'py', None)
    mask_spec = P(('batch', 'px'), 'py')
    whole = P()
    npy, npx = mesh.shape['py'], mesh.shape['px']
    n = npy * npx

    def device_body(pair_blk, mask_blk, ln_in, w_in, b_in, ln_out, w_out, b_out):
        rows, cols, dim = pair_blk.shape
        hidden = w_out.shape[1]
        slots = hidden // n
        full = npx * rows
        nx = npx // 2
        n_far = max(1, n - (npy - (npy > 2)) * (nx - (nx > 2)) * 2)
        width = w_in.shape[2]
        gate_at = 4 * hidden
        vec = jnp.concatenate([ln_in, b_in[:, None, gate_at:], b_out[:, None], ln_out], axis=1)
        vec = jnp.broadcast_to(vec.astype(F32)[..., None], (*vec.shape, 128))
        bias = b_in.astype(F32)

        vmem = pl.BlockSpec(memory_space=pltpu.VMEM)
        smem = pl.BlockSpec(memory_space=pltpu.SMEM)
        out = pl.pallas_call(
            functools.partial(kernel, npy, npx),
            out_shape=jax.ShapeDtypeStruct((rows, dim, cols), BF16),
            in_specs=[vmem, vmem, vmem, vmem, smem, vmem],
            out_specs=vmem,
            scratch_shapes=[
                pltpu.VMEM((width, SUB * dim), BF16),
                pltpu.VMEM((slots, 4 * n * SUB, SUB * dim), BF16),
                pltpu.VMEM((GATE_ROWS * dim, GATE_ROWS * dim), BF16),
                pltpu.VMEM((SUB * dim, SUB * hidden), BF16),
                pltpu.VMEM((rows, dim, cols), BF16),
                pltpu.VMEM((2, SUB * max(4 * n, dim), cols), F32),
                pltpu.VMEM((SUB * hidden, cols), BF16),
                pltpu.VMEM((slots, n, 2, rows, cols), BF16),
                pltpu.VMEM((slots, 2, full, full), BF16),
                pltpu.VMEM((2 * rows, full), BF16),
                pltpu.VMEM((slots, full, full), F32),
                pltpu.VMEM((hidden, rows, cols), F32),
                pltpu.VMEM((slots, n_far, 2, rows, cols), BF16),
                pltpu.VMEM((slots, n_far, rows, cols), F32),
                *[pltpu.SemaphoreType.DMA((slots, n))] * 4,
                *[pltpu.SemaphoreType.DMA((slots, n_far))] * 4,
                pltpu.SemaphoreType.REGULAR,
            ],
            compiler_params=pltpu.CompilerParams(collective_id=0, has_side_effects=True, vmem_limit_bytes=67043328),
            name='triangle',
        )(jnp.swapaxes(pair_blk, 1, 2), mask_blk, w_in, w_out, bias, vec)
        return jnp.swapaxes(out, 1, 2)

    return jax.shard_map(device_body, mesh=mesh, in_specs=(pair_spec, mask_spec, whole, whole, whole, whole, whole, whole), out_specs=pair_spec, check_vma=False)
```

```python
import functools

import jax
import jax.numpy as jnp
from jax import lax
from jax.experimental import pallas as pl
from jax.experimental.pallas import tpu as pltpu
from jax.sharding import PartitionSpec as P

LN_EPS = 1e-5
SUB = 8
GATE_ROWS = 4
MESH = pl.DeviceIdType.MESH
BF16 = jnp.bfloat16
F32 = jnp.float32


def dot(lhs, rhs, dims=((1,), (0,))):
    return lax.dot_general(lhs, rhs, (dims, ((), ())), preferred_element_type=F32)


def tree_sum(parts):
    while len(parts) > 1:
        parts = [parts[k] + parts[k + 1] if k + 1 < len(parts) else parts[k] for k in range(0, len(parts), 2)]
    return parts[0]


def kernel(npy, npx, z_ref, mask_ref, w_in_ref, w_out_ref, vec_ref,
           out_ref, w_t, wab, wg, wo, zn, proj, xn, ab_out, ab_in, a_t, x_out, x_in,
           ab_hop, x_hop, ab_ss, ab_rs, x_ss, x_rs, ab_hr, ab_fs, x_hr, x_fs, free_sem):
    rows, dim, cols = z_ref.shape
    hidden = x_in.shape[0]
    width = w_in_ref.shape[2]
    n = npy * npx
    slots = hidden // n
    full = npx * rows
    tile = 2 * rows
    my_py, my_px = lax.axis_index('py'), lax.axis_index('px')
    my_x, my_core = my_px // 2, lax.rem(my_px, 2)
    nx = npx // 2

    def peer(off):
        f, t, e = off
        dpy = lax.rem(my_py + f, npy)
        dpx = 2 * lax.rem(my_x + t, nx) + lax.rem(my_core + e, 2)
        return dpy, dpx

    def lin(dev):
        return dev[0] * npx + dev[1]

    def dev_id(dev):
        return {'py': dev[0], 'px': dev[1]}

    me = (my_py, my_px)
    here = lin(me)
    ring_y, ring_x = npy > 2 and npy % 2 == 0, nx > 2 and nx % 2 == 0
    num_y, num_x = npy - ring_y, nx - ring_x
    num_far = 2 * (npy * nx - num_y * num_x)

    half = rows // 2
    ab_parts = [(0, 0, half), (0, half, half)] + [(s, 0, rows) for s in range(1, slots)]
    last = slots
    x_parts = [(s, 0, rows) for s in range(slots - 1)] + [(slots - 1, 0, half), (slots - 1, half, half)]

    def straight(k, size, ring):
        return k + lax.div(k, size // 2) if ring else k

    def each_near(body):
        @pl.loop(1, 2 * num_y * num_x)
        def _(k):
            step = lax.div(k, 2)
            f = straight(lax.rem(step + lax.div(step, num_x), num_y), npy, ring_y)
            t = straight(lax.rem(step, num_x), nx, ring_x)
            body(peer((f, t, lax.rem(k, 2))))

    def each_far(p, body):
        def visit(k, f, t, e, over_y, over_x):
            turn = 1 - 2 * lax.rem(p + e, 2)
            f1 = lax.rem(turn + npy, npy) if over_y else f
            t1 = lax.rem(turn + nx, nx) if over_x else t
            f2, t2 = lax.rem(f - f1 + npy, npy), lax.rem(t - t1 + nx, nx)
            origin = peer((lax.rem(npy - f1, npy), lax.rem(nx - t1, nx), e))
            body(k, peer((f, t, e)), peer((f1, t1, e)), origin, peer((f2, t2, 0)))

        if ring_x:
            @pl.loop(0, 2 * num_y)
            def _(k):
                visit(k, straight(lax.div(k, 2), npy, ring_y), nx // 2, lax.rem(k, 2), False, True)
        if ring_y:
            @pl.loop(0, 2 * num_x)
            def _(k):
                visit(2 * num_y * ring_x + k, npy // 2, straight(lax.div(k, 2), nx, ring_x), lax.rem(k, 2), True, False)
        if ring_x and ring_y:
            @pl.loop(0, 2)
            def _(k):
                visit(2 * (num_y + num_x) + k, npy // 2, nx // 2, k, True, True)

    def each_other(body):
        @pl.loop(1, n)
        def _(k):
            dev = lax.rem(here + k, n)
            body((dev // npx, lax.rem(dev, npx)))

    def signal_all(sem):
        each_other(lambda dev: pl.semaphore_signal(sem, inc=1, device_id=dev_id(dev), device_id_type=MESH))

    def at_rows(dev, first=0, count=rows):
        return pl.ds(pl.multiple_of(dev[1] * rows + first, count), count)

    def at_cols(dev):
        return pl.ds(pl.multiple_of(dev[0] * cols, cols), cols)

    def remote(src, dst, send_sem, recv_sem, dev):
        return pltpu.make_async_remote_copy(src_ref=src, dst_ref=dst, send_sem=send_sem, recv_sem=recv_sem,
                                            device_id=dev_id(dev), device_id_type=MESH)

    def ab_place(p, src):
        s, first, count = ab_parts[p]
        return ab_in.at[s, :, at_rows(src, first, count), at_cols(src)]

    def ab_from(p, dst):
        s, first, count = ab_parts[p]
        return ab_out.at[s, lin(dst), :, pl.ds(first, count), :]

    def ab_stop(p, k):
        s, first, count = ab_parts[p]
        return ab_hop.at[s, k, :, pl.ds(first, count), :]

    def x_place(p, src):
        s, first, count = x_parts[p]
        return x_in.at[s * n + lin(src), pl.ds(first, count), :]

    def x_from(p, dst):
        s, first, count = x_parts[p]
        return x_out.at[s, at_rows(dst, first, count), at_cols(dst)]

    def x_stop(p, k):
        s, first, count = x_parts[p]
        return x_hop.at[s, k, pl.ds(first, count), :]

    def ab_copy(p, src, dst):
        return remote(ab_from(p, dst), ab_place(p, src), ab_ss.at[p, lin(dst)], ab_rs.at[p, lin(src)], dst)

    def x_copy(p, src, dst):
        return remote(x_from(p, dst), x_place(p, src), x_ss.at[p, lin(dst)], x_rs.at[p, lin(src)], dst)

    def ab_first(p, k, dst, stop):
        return remote(ab_from(p, dst), ab_stop(p, k), ab_ss.at[p, lin(dst)], ab_hr.at[p, k], stop)

    def ab_second(p, k, origin, dst):
        return remote(ab_stop(p, k), ab_place(p, origin), ab_fs.at[p, k], ab_rs.at[p, lin(origin)], dst)

    def x_first(p, k, dst, stop):
        return remote(x_from(p, dst), x_stop(p, k), x_ss.at[p, lin(dst)], x_hr.at[p, k], stop)

    def x_second(p, k, origin, dst):
        return remote(x_stop(p, k), x_place(p, origin), x_fs.at[p, k], x_rs.at[p, lin(origin)], dst)

    def ab_left(p, k):
        return remote(ab_stop(p, k), ab_place(p, me), ab_fs.at[p, k], ab_rs.at[p, here], me)

    def x_left(p, k):
        return remote(x_stop(p, k), x_place(p, me), x_fs.at[p, k], x_rs.at[p, here], me)

    def pass_on(first, second, p):
        def body(k, dst, stop, origin, onward):
            first(p, k, dst, stop).wait_recv()
            second(p, k, origin, onward).start()
        each_far(p, body)

    def send(first, copy, p):
        each_far(p, lambda k, dst, stop, origin, onward: first(p, k, dst, stop).start())
        each_near(lambda dev: copy(p, me, dev).start())

    def wait_forwards(left, parts):
        for p in parts:
            @pl.loop(0, num_far)
            def _(k):
                left(p, k).wait_send()

    def wait_sent(copy, parts):
        for p in range(len(parts)):
            each_other(lambda dev: copy(p, me, dev).wait_send())

    def iota(shape, axis):
        return lax.broadcasted_iota(jnp.int32, shape, axis)

    def spread_in(u):
        wide = (dim, SUB * dim)
        pick = (lax.rem(iota(wide, 1), dim) == iota(wide, 0)).astype(F32).astype(BF16)
        w_t[...] = dot(w_in_ref[u], pick, ((0,), (0,))).astype(BF16)
        big = (n * SUB, SUB * dim)
        keep = lax.rem(iota(big, 0), SUB) == iota(big, 1) // dim
        sel = (n * SUB, width)
        for s in range(slots):
            for k in range(4):
                first = k * hidden + s * n
                rep = (iota(sel, 0) // SUB + first == iota(sel, 1)).astype(F32).astype(BF16)
                wab[s, pl.ds(k * n * SUB, n * SUB), :] = jnp.where(keep, dot(rep, w_t[...]), 0.0).astype(BF16)

    def spread_out(u):
        gate_w = w_t[pl.ds(4 * hidden, dim), pl.ds(0, GATE_ROWS * dim)].astype(F32)
        lane = iota(gate_w.shape, 1)
        for r in range(GATE_ROWS):
            wg[pl.ds(r * dim, dim), :] = jnp.where(lane // dim == r, gate_w, 0.0).astype(BF16)
        wide = (hidden, SUB * hidden)
        pick = (iota(wide, 1) // SUB == iota(wide, 0)).astype(F32).astype(BF16)
        out_w = dot(w_out_ref[u], pick, ((0,), (0,)))
        lane = iota(out_w.shape, 1)
        for r in range(SUB):
            wo[pl.ds(r * dim, dim), :] = jnp.where(lax.rem(lane, SUB) == r, out_w, 0.0).astype(BF16)

    def normalize(src_ref, u, start, count):
        gain, shift = vec_ref[u, 0], vec_ref[u, 1]

        @pl.loop(start, start + count, unroll=4)
        def _(i):
            for h in range(cols // 128):
                lanes = pl.ds(h * 128, 128)
                val = src_ref[i, :, lanes].astype(F32)
                cen = val - jnp.mean(val, axis=0, keepdims=True)
                var = jnp.mean(cen * cen, axis=0, keepdims=True)
                zn[i, :, lanes] = (cen * lax.rsqrt(var + LN_EPS) * gain + shift).astype(BF16)

    def project(u, p):
        s, start, count = ab_parts[p]

        @pl.loop(start // (2 * SUB), (start + count) // (2 * SUB))
        def _(g):
            for h in range(2):
                rhs = zn[pl.ds(g * 2 * SUB + h * SUB, SUB)].reshape(SUB * dim, cols)
                proj[h, pl.ds(0, 4 * n * SUB), :] = dot(wab[s], rhs)
            at = pl.ds(pl.multiple_of(g * 2 * SUB, 2 * SUB), 2 * SUB)
            mask = mask_ref[at, :].astype(F32)

            @pl.loop(0, n, unroll=4)
            def _(d):
                for op in range(2):
                    bias_g, bias_p = [jnp.concatenate([vec_ref[u, 2 + 2 * op + k, pl.ds(s * n + d, 1), :]] * (cols // 128), axis=1) for k in range(2)]
                    g_at = pl.ds(pl.multiple_of((2 * op * n + d) * SUB, SUB), SUB)
                    p_at = pl.ds(pl.multiple_of(((2 * op + 1) * n + d) * SUB, SUB), SUB)
                    gate = jnp.concatenate([proj[0, g_at, :], proj[1, g_at, :]], axis=0) + bias_g
                    lin_p = jnp.concatenate([proj[0, p_at, :], proj[1, p_at, :]], axis=0) + bias_p
                    ab_out[s, d, op, at, :] = (mask * jax.nn.sigmoid(gate) * lin_p).astype(BF16)

    def send_ab(p):
        s, start, count = ab_parts[p]
        send(ab_first, ab_copy, p)
        ab_in[s, :, at_rows(me, start, count), at_cols(me)] = ab_out[s, here, :, pl.ds(start, count), :]

    def products(u, s):
        for t in range(nx):
            m = lax.rem(my_x + t, nx)
            m_at = pl.ds(pl.multiple_of(m * tile, tile), tile)
            if u == 0:
                lhs_ref = ab_in.at[s, 0, m_at, :]
            else:
                a_t[...] = ab_in[s, 0, :, m_at].T
                lhs_ref = a_t

            @pl.loop(0, full // cols)
            def _(q):
                q_at = pl.ds(pl.multiple_of(q * cols, cols), cols)
                if u == 0:
                    x_out[s, m_at, q_at] = dot(lhs_ref[...], ab_in[s, 1, q_at, :], ((1,), (1,)))
                else:
                    x_out[s, m_at, q_at] = dot(lhs_ref[...], ab_in[s, 1, :, q_at])

        for p, part in enumerate(x_parts):
            if part[0] == s and p < last:
                send(x_first, x_copy, p)
        x_in[s * n + here] = x_out[s, at_rows(me), at_cols(me)]

    def finish(src_ref, u, start, count):
        @pl.loop(start // SUB, (start + count) // SUB)
        def _(g):
            at = pl.ds(pl.multiple_of(g * SUB, SUB), SUB)
            for h in range(cols // 128):
                lanes = pl.ds(h * 128, 128)
                avg = tree_sum([x_in[c, at, lanes] for c in range(hidden)]) * (1.0 / hidden)
                var = tree_sum([jnp.square(x_in[c, at, lanes] - avg) for c in range(hidden)]) * (1.0 / hidden)
                inv = lax.rsqrt(var + LN_EPS)
                for c in range(0, hidden, 2):
                    pair = [(x_in[k, at, lanes] - avg) * inv * vec_ref[u, 8, pl.ds(k, 1), :] + vec_ref[u, 9, pl.ds(k, 1), :] for k in (c, c + 1)]
                    xn[pl.ds(c * SUB, 2 * SUB), lanes] = jnp.concatenate(pair, axis=0).astype(BF16)
            proj[0, pl.ds(0, SUB * dim), :] = dot(wo[...], xn[...])
            for k in range(SUB // GATE_ROWS):
                rhs = zn[pl.ds(g * SUB + k * GATE_ROWS, GATE_ROWS)].reshape(GATE_ROWS * dim, cols)
                proj[1, pl.ds(k * GATE_ROWS * dim, GATE_ROWS * dim), :] = dot(wg[...], rhs)

            @pl.loop(0, SUB, unroll=4)
            def _(r):
                r_at = pl.ds(pl.multiple_of(r * dim, dim), dim)
                for h in range(cols // 128):
                    lanes = pl.ds(h * 128, 128)
                    gate = jax.nn.sigmoid(proj[1, r_at, lanes] + vec_ref[u, 6])
                    upd = proj[0, r_at, lanes] + vec_ref[u, 7]
                    out_ref[g * SUB + r, :, lanes] = (src_ref[g * SUB + r, :, lanes].astype(F32) + gate * upd).astype(BF16)

    barrier = pltpu.get_barrier_semaphore()
    signal_all(barrier)
    early_x, last_x = list(range(slots - 1)), [last - 1, last]

    def begin(src_ref, u, h):
        normalize(src_ref, u, h * half, half)
        project(u, h)

    spread_in(0)
    begin(z_ref, 0, 0)
    pl.semaphore_wait(barrier, n - 1)
    for u in range(2):
        src_ref = z_ref if u == 0 else out_ref
        if u == 0:
            send_ab(0)
            begin(src_ref, u, 1)
            send_ab(1)
        for p in range(2, len(ab_parts)):
            project(u, p)
            if u == 1 and p == len(ab_parts) - 1:
                wait_forwards(x_left, last_x)
            send_ab(p)
        spread_out(u)
        if u == 1:
            wait_sent(x_copy, x_parts)
        for s in range(slots):
            for p, part in enumerate(ab_parts):
                if part[0] == s:
                    pass_on(ab_first, ab_second, p)
            for p, part in enumerate(ab_parts):
                if part[0] == s:
                    each_other(lambda dev: ab_copy(p, dev, me).wait_recv())
            products(u, s)
        wait_forwards(ab_left, range(len(ab_parts)))
        wait_sent(ab_copy, ab_parts)
        if u == 0:
            signal_all(free_sem)
            spread_in(1)
        for p in range(last):
            pass_on(x_first, x_second, p)
        send(x_first, x_copy, last)
        for p in range(last):
            each_other(lambda dev: x_copy(p, dev, me).wait_recv())
        finish(src_ref, u, 0, half)
        pass_on(x_first, x_second, last)
        if u == 0:
            begin(out_ref, 1, 0)
            pl.semaphore_wait(free_sem, n - 1)
            send_ab(0)
        each_other(lambda dev: x_copy(last, dev, me).wait_recv())
        finish(src_ref, u, half, half)
        if u == 0:
            begin(out_ref, 1, 1)
            wait_forwards(x_left, early_x if slots > 1 else last_x)
            send_ab(1)
    wait_sent(x_copy, x_parts)
    wait_forwards(x_left, early_x + last_x)


def solution(mesh):
    pair_spec = P(('batch', 'px'), 'py', None)
    mask_spec = P(('batch', 'px'), 'py')
    whole = P()
    npy, npx = mesh.shape['py'], mesh.shape['px']
    n = npy * npx

    def device_body(pair_blk, mask_blk, ln_in, w_in, b_in, ln_out, w_out, b_out):
        rows, cols, dim = pair_blk.shape
        hidden = w_out.shape[1]
        slots = hidden // n
        full = npx * rows
        nx = npx // 2
        n_far = max(1, n - (npy - (npy > 2)) * (nx - (nx > 2)) * 2)
        width = w_in.shape[2]
        vec = jnp.concatenate([ln_in, b_in.reshape(b_in.shape[0], -1, dim), b_out[:, None], ln_out], axis=1)
        vec = jnp.broadcast_to(vec.astype(F32)[..., None], (*vec.shape, 128))

        vmem = pl.BlockSpec(memory_space=pltpu.VMEM)
        out = pl.pallas_call(
            functools.partial(kernel, npy, npx),
            out_shape=jax.ShapeDtypeStruct((rows, dim, cols), BF16),
            in_specs=[vmem] * 5,
            out_specs=vmem,
            scratch_shapes=[
                pltpu.VMEM((width, SUB * dim), BF16),
                pltpu.VMEM((slots, 4 * n * SUB, SUB * dim), BF16),
                pltpu.VMEM((GATE_ROWS * dim, GATE_ROWS * dim), BF16),
                pltpu.VMEM((SUB * dim, SUB * hidden), BF16),
                pltpu.VMEM((rows, dim, cols), BF16),
                pltpu.VMEM((2, SUB * max(4 * n, dim), cols), F32),
                pltpu.VMEM((SUB * hidden, cols), BF16),
                pltpu.VMEM((slots, n, 2, rows, cols), BF16),
                pltpu.VMEM((slots, 2, full, full), BF16),
                pltpu.VMEM((2 * rows, full), BF16),
                pltpu.VMEM((slots, full, full), F32),
                pltpu.VMEM((hidden, rows, cols), F32),
                pltpu.VMEM((slots, n_far, 2, rows, cols), BF16),
                pltpu.VMEM((slots, n_far, rows, cols), F32),
                *[pltpu.SemaphoreType.DMA((slots + 1, n))] * 4,
                *[pltpu.SemaphoreType.DMA((slots + 1, n_far))] * 4,
                pltpu.SemaphoreType.REGULAR,
            ],
            compiler_params=pltpu.CompilerParams(collective_id=0, has_side_effects=True, vmem_limit_bytes=67043328),
            name='triangle',
        )(jnp.swapaxes(pair_blk, 1, 2), mask_blk, w_in, w_out, vec)
        return jnp.swapaxes(out, 1, 2)

    return jax.shard_map(device_body, mesh=mesh, in_specs=(pair_spec, mask_spec, whole, whole, whole, whole, whole, whole), out_specs=pair_spec, check_vma=False)
```

```python
import functools

import jax
import jax.numpy as jnp
from jax import lax
from jax.experimental import pallas as pl
from jax.experimental.pallas import tpu as pltpu
from jax.sharding import PartitionSpec as P

LN_EPS = 1e-5
SUB = 8
GATE_ROWS = 4
MESH = pl.DeviceIdType.MESH
BF16 = jnp.bfloat16
F32 = jnp.float32


def dot(lhs, rhs, dims=((1,), (0,))):
    return lax.dot_general(lhs, rhs, (dims, ((), ())), preferred_element_type=F32)


def tree_sum(parts):
    while len(parts) > 1:
        parts = [parts[k] + parts[k + 1] if k + 1 < len(parts) else parts[k] for k in range(0, len(parts), 2)]
    return parts[0]


def kernel(npy, npx, z_ref, mask_ref, w_in_ref, w_out_ref, vec_ref,
           out_ref, w_t, wab, wg, wo, zn, proj, xn, ab_out, ab_in, a_t, x_out, x_in,
           ab_hop, x_hop, ab_ss, ab_rs, x_ss, x_rs, ab_hr, ab_fs, x_hr, x_fs, free_sem):
    rows, dim, cols = z_ref.shape
    hidden = x_in.shape[0]
    width = w_in_ref.shape[2]
    n = npy * npx
    slots = hidden // n
    full = npx * rows
    tile = 2 * rows
    my_py, my_px = lax.axis_index('py'), lax.axis_index('px')
    my_x, my_core = my_px // 2, lax.rem(my_px, 2)
    nx = npx // 2

    def peer(off):
        f, t, e = off
        dpy = lax.rem(my_py + f, npy)
        dpx = 2 * lax.rem(my_x + t, nx) + lax.rem(my_core + e, 2)
        return dpy, dpx

    def lin(dev):
        return dev[0] * npx + dev[1]

    def dev_id(dev):
        return {'py': dev[0], 'px': dev[1]}

    me = (my_py, my_px)
    here = lin(me)
    ring_y, ring_x = npy > 2 and npy % 2 == 0, nx > 2 and nx % 2 == 0
    num_y, num_x = npy - ring_y, nx - ring_x
    halfway = 2 * (npy * nx - num_y * num_x)
    corners = 4 if ring_x and ring_y else 0
    num_far = halfway + corners

    half = rows // 2
    ab_parts = [(0, 0, half), (0, half, half)] + [(s, 0, rows) for s in range(1, slots)]
    last = slots
    x_parts = [(s, 0, rows) for s in range(slots - 1)] + [(slots - 1, 0, half), (slots - 1, half, half)]

    def straight(k, size, ring):
        return k + lax.div(k, size // 2) if ring else k

    def each_near(body):
        @pl.loop(1, 2 * num_y * num_x)
        def _(k):
            step = lax.div(k, 2)
            f = straight(lax.rem(step + lax.div(step, num_x), num_y), npy, ring_y)
            t = straight(lax.rem(step, num_x), nx, ring_x)
            e = lax.rem(k, 2)
            if corners:
                is_corner = (e == 1) & ((f == 1) | (f == npy - 1)) & ((t == 1) | (t == nx - 1))
                pl.when(jnp.logical_not(is_corner))(lambda: body(peer((f, t, e))))
            else:
                body(peer((f, t, e)))

    def each_far(p, body):
        def visit(k, f, t, e, over_y, over_x):
            turn = 1 - 2 * lax.rem(p + e, 2)
            f1 = lax.rem(turn + npy, npy) if over_y else f
            t1 = lax.rem(turn + nx, nx) if over_x else t
            stop(k, f, t, e, f1, t1)

        def stop(k, f, t, e, f1, t1):
            f2, t2 = lax.rem(f - f1 + npy, npy), lax.rem(t - t1 + nx, nx)
            origin = peer((lax.rem(npy - f1, npy), lax.rem(nx - t1, nx), e))
            body(k, peer((f, t, e)), peer((f1, t1, e)), origin, peer((f2, t2, 0)))

        if corners:
            @pl.loop(0, corners)
            def _(k):
                f, t = 1 + (npy - 2) * lax.div(k, 2), 1 + (nx - 2) * lax.rem(k, 2)
                stop(halfway + k, f, t, 1, f, 0)

        if ring_x:
            @pl.loop(0, 2 * num_y)
            def _(k):
                visit(k, straight(lax.div(k, 2), npy, ring_y), nx // 2, lax.rem(k, 2), False, True)
        if ring_y:
            @pl.loop(0, 2 * num_x)
            def _(k):
                visit(2 * num_y * ring_x + k, npy // 2, straight(lax.div(k, 2), nx, ring_x), lax.rem(k, 2), True, False)
        if ring_x and ring_y:
            @pl.loop(0, 2)
            def _(k):
                visit(2 * (num_y + num_x) + k, npy // 2, nx // 2, k, True, True)

    def each_other(body):
        @pl.loop(1, n)
        def _(k):
            dev = lax.rem(here + k, n)
            body((dev // npx, lax.rem(dev, npx)))

    def signal_all(sem):
        each_other(lambda dev: pl.semaphore_signal(sem, inc=1, device_id=dev_id(dev), device_id_type=MESH))

    def at_rows(dev, first=0, count=rows):
        return pl.ds(pl.multiple_of(dev[1] * rows + first, count), count)

    def at_cols(dev):
        return pl.ds(pl.multiple_of(dev[0] * cols, cols), cols)

    def remote(src, dst, send_sem, recv_sem, dev):
        return pltpu.make_async_remote_copy(src_ref=src, dst_ref=dst, send_sem=send_sem, recv_sem=recv_sem,
                                            device_id=dev_id(dev), device_id_type=MESH)

    def ab_place(p, src):
        s, first, count = ab_parts[p]
        return ab_in.at[s, :, at_rows(src, first, count), at_cols(src)]

    def ab_from(p, dst):
        s, first, count = ab_parts[p]
        return ab_out.at[s, lin(dst), :, pl.ds(first, count), :]

    def ab_stop(p, k):
        s, first, count = ab_parts[p]
        return ab_hop.at[s, k, :, pl.ds(first, count), :]

    def x_place(p, src):
        s, first, count = x_parts[p]
        return x_in.at[s * n + lin(src), pl.ds(first, count), :]

    def x_from(p, dst):
        s, first, count = x_parts[p]
        return x_out.at[s, at_rows(dst, first, count), at_cols(dst)]

    def x_stop(p, k):
        s, first, count = x_parts[p]
        return x_hop.at[s, k, pl.ds(first, count), :]

    def ab_copy(p, src, dst):
        return remote(ab_from(p, dst), ab_place(p, src), ab_ss.at[p, lin(dst)], ab_rs.at[p, lin(src)], dst)

    def x_copy(p, src, dst):
        return remote(x_from(p, dst), x_place(p, src), x_ss.at[p, lin(dst)], x_rs.at[p, lin(src)], dst)

    def ab_first(p, k, dst, stop):
        return remote(ab_from(p, dst), ab_stop(p, k), ab_ss.at[p, lin(dst)], ab_hr.at[p, k], stop)

    def ab_second(p, k, origin, dst):
        return remote(ab_stop(p, k), ab_place(p, origin), ab_fs.at[p, k], ab_rs.at[p, lin(origin)], dst)

    def x_first(p, k, dst, stop):
        return remote(x_from(p, dst), x_stop(p, k), x_ss.at[p, lin(dst)], x_hr.at[p, k], stop)

    def x_second(p, k, origin, dst):
        return remote(x_stop(p, k), x_place(p, origin), x_fs.at[p, k], x_rs.at[p, lin(origin)], dst)

    def ab_left(p, k):
        return remote(ab_stop(p, k), ab_place(p, me), ab_fs.at[p, k], ab_rs.at[p, here], me)

    def x_left(p, k):
        return remote(x_stop(p, k), x_place(p, me), x_fs.at[p, k], x_rs.at[p, here], me)

    def pass_on(first, second, p):
        def body(k, dst, stop, origin, onward):
            first(p, k, dst, stop).wait_recv()
            second(p, k, origin, onward).start()
        each_far(p, body)

    def send(first, copy, p):
        each_far(p, lambda k, dst, stop, origin, onward: first(p, k, dst, stop).start())
        each_near(lambda dev: copy(p, me, dev).start())

    def wait_forwards(left, parts):
        for p in parts:
            @pl.loop(0, num_far)
            def _(k):
                left(p, k).wait_send()

    def wait_sent(copy, parts):
        for p in range(len(parts)):
            each_other(lambda dev: copy(p, me, dev).wait_send())

    def iota(shape, axis):
        return lax.broadcasted_iota(jnp.int32, shape, axis)

    def spread_in(u):
        wide = (dim, SUB * dim)
        pick = (lax.rem(iota(wide, 1), dim) == iota(wide, 0)).astype(F32).astype(BF16)
        w_t[...] = dot(w_in_ref[u], pick, ((0,), (0,))).astype(BF16)
        big = (n * SUB, SUB * dim)
        keep = lax.rem(iota(big, 0), SUB) == iota(big, 1) // dim
        sel = (n * SUB, width)
        for s in range(slots):
            for k in range(4):
                first = k * hidden + s * n
                rep = (iota(sel, 0) // SUB + first == iota(sel, 1)).astype(F32).astype(BF16)
                wab[s, pl.ds(k * n * SUB, n * SUB), :] = jnp.where(keep, dot(rep, w_t[...]), 0.0).astype(BF16)

    def spread_out(u):
        gate_w = w_t[pl.ds(4 * hidden, dim), pl.ds(0, GATE_ROWS * dim)].astype(F32)
        lane = iota(gate_w.shape, 1)
        for r in range(GATE_ROWS):
            wg[pl.ds(r * dim, dim), :] = jnp.where(lane // dim == r, gate_w, 0.0).astype(BF16)
        wide = (hidden, SUB * hidden)
        pick = (iota(wide, 1) // SUB == iota(wide, 0)).astype(F32).astype(BF16)
        out_w = dot(w_out_ref[u], pick, ((0,), (0,)))
        lane = iota(out_w.shape, 1)
        for r in range(SUB):
            wo[pl.ds(r * dim, dim), :] = jnp.where(lax.rem(lane, SUB) == r, out_w, 0.0).astype(BF16)

    def normalize(src_ref, u, start, count):
        gain, shift = vec_ref[u, 0], vec_ref[u, 1]

        @pl.loop(start, start + count, unroll=4)
        def _(i):
            for h in range(cols // 128):
                lanes = pl.ds(h * 128, 128)
                val = src_ref[i, :, lanes].astype(F32)
                cen = val - jnp.mean(val, axis=0, keepdims=True)
                var = jnp.mean(cen * cen, axis=0, keepdims=True)
                zn[i, :, lanes] = (cen * lax.rsqrt(var + LN_EPS) * gain + shift).astype(BF16)

    def project(u, p):
        s, start, count = ab_parts[p]

        @pl.loop(start // (2 * SUB), (start + count) // (2 * SUB))
        def _(g):
            for h in range(2):
                rhs = zn[pl.ds(g * 2 * SUB + h * SUB, SUB)].reshape(SUB * dim, cols)
                proj[h, pl.ds(0, 4 * n * SUB), :] = dot(wab[s], rhs)
            at = pl.ds(pl.multiple_of(g * 2 * SUB, 2 * SUB), 2 * SUB)
            mask = mask_ref[at, :].astype(F32)

            @pl.loop(0, n, unroll=4)
            def _(d):
                for op in range(2):
                    bias_g, bias_p = [jnp.concatenate([vec_ref[u, 2 + 2 * op + k, pl.ds(s * n + d, 1), :]] * (cols // 128), axis=1) for k in range(2)]
                    g_at = pl.ds(pl.multiple_of((2 * op * n + d) * SUB, SUB), SUB)
                    p_at = pl.ds(pl.multiple_of(((2 * op + 1) * n + d) * SUB, SUB), SUB)
                    gate = jnp.concatenate([proj[0, g_at, :], proj[1, g_at, :]], axis=0) + bias_g
                    lin_p = jnp.concatenate([proj[0, p_at, :], proj[1, p_at, :]], axis=0) + bias_p
                    ab_out[s, d, op, at, :] = (mask * jax.nn.sigmoid(gate) * lin_p).astype(BF16)

    def send_ab(p):
        s, start, count = ab_parts[p]
        send(ab_first, ab_copy, p)
        ab_in[s, :, at_rows(me, start, count), at_cols(me)] = ab_out[s, here, :, pl.ds(start, count), :]

    def products(u, s):
        for t in range(nx):
            m = lax.rem(my_x + t, nx)
            m_at = pl.ds(pl.multiple_of(m * tile, tile), tile)
            if u == 0:
                lhs_ref = ab_in.at[s, 0, m_at, :]
            else:
                a_t[...] = ab_in[s, 0, :, m_at].T
                lhs_ref = a_t

            @pl.loop(0, full // cols)
            def _(q):
                q_at = pl.ds(pl.multiple_of(q * cols, cols), cols)
                if u == 0:
                    x_out[s, m_at, q_at] = dot(lhs_ref[...], ab_in[s, 1, q_at, :], ((1,), (1,)))
                else:
                    x_out[s, m_at, q_at] = dot(lhs_ref[...], ab_in[s, 1, :, q_at])

        for p, part in enumerate(x_parts):
            if part[0] == s and p < last:
                send(x_first, x_copy, p)
        x_in[s * n + here] = x_out[s, at_rows(me), at_cols(me)]

    def finish(src_ref, u, start, count):
        @pl.loop(start // SUB, (start + count) // SUB)
        def _(g):
            at = pl.ds(pl.multiple_of(g * SUB, SUB), SUB)
            for h in range(cols // 128):
                lanes = pl.ds(h * 128, 128)
                avg = tree_sum([x_in[c, at, lanes] for c in range(hidden)]) * (1.0 / hidden)
                var = tree_sum([jnp.square(x_in[c, at, lanes] - avg) for c in range(hidden)]) * (1.0 / hidden)
                inv = lax.rsqrt(var + LN_EPS)
                for c in range(0, hidden, 2):
                    pair = [(x_in[k, at, lanes] - avg) * inv * vec_ref[u, 8, pl.ds(k, 1), :] + vec_ref[u, 9, pl.ds(k, 1), :] for k in (c, c + 1)]
                    xn[pl.ds(c * SUB, 2 * SUB), lanes] = jnp.concatenate(pair, axis=0).astype(BF16)
            proj[0, pl.ds(0, SUB * dim), :] = dot(wo[...], xn[...])
            for k in range(SUB // GATE_ROWS):
                rhs = zn[pl.ds(g * SUB + k * GATE_ROWS, GATE_ROWS)].reshape(GATE_ROWS * dim, cols)
                proj[1, pl.ds(k * GATE_ROWS * dim, GATE_ROWS * dim), :] = dot(wg[...], rhs)

            @pl.loop(0, SUB, unroll=4)
            def _(r):
                r_at = pl.ds(pl.multiple_of(r * dim, dim), dim)
                for h in range(cols // 128):
                    lanes = pl.ds(h * 128, 128)
                    gate = jax.nn.sigmoid(proj[1, r_at, lanes] + vec_ref[u, 6])
                    upd = proj[0, r_at, lanes] + vec_ref[u, 7]
                    out_ref[g * SUB + r, :, lanes] = (src_ref[g * SUB + r, :, lanes].astype(F32) + gate * upd).astype(BF16)

    barrier = pltpu.get_barrier_semaphore()
    signal_all(barrier)
    early_x, last_x = list(range(slots - 1)), [last - 1, last]

    def begin(src_ref, u, h):
        normalize(src_ref, u, h * half, half)
        project(u, h)

    spread_in(0)
    begin(z_ref, 0, 0)
    pl.semaphore_wait(barrier, n - 1)
    for u in range(2):
        src_ref = z_ref if u == 0 else out_ref
        if u == 0:
            send_ab(0)
            begin(src_ref, u, 1)
            send_ab(1)
        for p in range(2, len(ab_parts)):
            project(u, p)
            if u == 1 and p == len(ab_parts) - 1:
                wait_forwards(x_left, last_x)
            send_ab(p)
        spread_out(u)
        if u == 1:
            wait_sent(x_copy, x_parts)
        for s in range(slots):
            for p, part in enumerate(ab_parts):
                if part[0] == s:
                    pass_on(ab_first, ab_second, p)
            for p, part in enumerate(ab_parts):
                if part[0] == s:
                    each_other(lambda dev: ab_copy(p, dev, me).wait_recv())
            products(u, s)
        wait_forwards(ab_left, range(len(ab_parts)))
        wait_sent(ab_copy, ab_parts)
        if u == 0:
            signal_all(free_sem)
            spread_in(1)
        for p in range(last):
            pass_on(x_first, x_second, p)
        send(x_first, x_copy, last)
        for p in range(last):
            each_other(lambda dev: x_copy(p, dev, me).wait_recv())
        finish(src_ref, u, 0, half)
        pass_on(x_first, x_second, last)
        if u == 0:
            begin(out_ref, 1, 0)
            pl.semaphore_wait(free_sem, n - 1)
            send_ab(0)
        each_other(lambda dev: x_copy(last, dev, me).wait_recv())
        finish(src_ref, u, half, half)
        if u == 0:
            begin(out_ref, 1, 1)
            wait_forwards(x_left, early_x if slots > 1 else last_x)
            send_ab(1)
    wait_sent(x_copy, x_parts)
    wait_forwards(x_left, early_x + last_x)


def solution(mesh):
    pair_spec = P(('batch', 'px'), 'py', None)
    mask_spec = P(('batch', 'px'), 'py')
    whole = P()
    npy, npx = mesh.shape['py'], mesh.shape['px']
    n = npy * npx

    def device_body(pair_blk, mask_blk, ln_in, w_in, b_in, ln_out, w_out, b_out):
        rows, cols, dim = pair_blk.shape
        hidden = w_out.shape[1]
        slots = hidden // n
        full = npx * rows
        nx = npx // 2
        n_far = n // 2 + 2 if npy > 2 and nx > 2 else n
        width = w_in.shape[2]
        vec = jnp.concatenate([ln_in, b_in.reshape(b_in.shape[0], -1, dim), b_out[:, None], ln_out], axis=1)
        vec = jnp.broadcast_to(vec.astype(F32)[..., None], (*vec.shape, 128))

        vmem = pl.BlockSpec(memory_space=pltpu.VMEM)
        out = pl.pallas_call(
            functools.partial(kernel, npy, npx),
            out_shape=jax.ShapeDtypeStruct((rows, dim, cols), BF16),
            in_specs=[vmem] * 5,
            out_specs=vmem,
            scratch_shapes=[
                pltpu.VMEM((width, SUB * dim), BF16),
                pltpu.VMEM((slots, 4 * n * SUB, SUB * dim), BF16),
                pltpu.VMEM((GATE_ROWS * dim, GATE_ROWS * dim), BF16),
                pltpu.VMEM((SUB * dim, SUB * hidden), BF16),
                pltpu.VMEM((rows, dim, cols), BF16),
                pltpu.VMEM((2, SUB * max(4 * n, dim), cols), F32),
                pltpu.VMEM((SUB * hidden, cols), BF16),
                pltpu.VMEM((slots, n, 2, rows, cols), BF16),
                pltpu.VMEM((slots, 2, full, full), BF16),
                pltpu.VMEM((2 * rows, full), BF16),
                pltpu.VMEM((slots, full, full), F32),
                pltpu.VMEM((hidden, rows, cols), F32),
                pltpu.VMEM((slots, n_far, 2, rows, cols), BF16),
                pltpu.VMEM((slots, n_far, rows, cols), F32),
                *[pltpu.SemaphoreType.DMA((slots + 1, n))] * 4,
                *[pltpu.SemaphoreType.DMA((slots + 1, n_far))] * 4,
                pltpu.SemaphoreType.REGULAR,
            ],
            compiler_params=pltpu.CompilerParams(collective_id=0, has_side_effects=True, vmem_limit_bytes=67043328),
            name='triangle',
        )(jnp.swapaxes(pair_blk, 1, 2), mask_blk, w_in, w_out, vec)
        return jnp.swapaxes(out, 1, 2)

    return jax.shard_map(device_body, mesh=mesh, in_specs=(pair_spec, mask_spec, whole, whole, whole, whole, whole, whole), out_specs=pair_spec, check_vma=False)
```
